32 devices in a mesh: rep: 4 (over z), shard: 8 (over y, x, core).
Axes of the slice: x: 2, y: 2, z: 4, core: 2. Of those that a mesh axis runs over, the one named last changes fastest.
Arguments:
- tokens: bfloat16 [32, 1024, 768], P(('rep', 'shard')), may hold values from -6 to 6
- cotangent: bfloat16 [32, 1024, 768], P(('rep', 'shard')), may hold values from -6 to 6
- lengths: int32 [4, 8], P('rep'), may hold values from 1 to 1024, 5120 in all within a row
- dealing: int32 [4, 8], P('rep'), may hold values from 0 to 7, each once within a row
- drop_flags: int32 [4, 8], P('rep'), may hold values 0 or 1
- query_weight: float32 [768, 768], P('shard'), may hold values from -0.3125 to 0.3125
- key_weight: float32 [768, 768], P('shard'), may hold values from -0.21875 to 0.21875
- value_weight: float32 [768, 768], P('shard'), may hold values from -0.21875 to 0.21875
- out_weight: float32 [768, 768], P('shard'), may hold values from -0.875 to 0.875
- up_weight: float32 [768, 3072], P('shard'), may hold values from -0.21875 to 0.21875
- down_weight: float32 [3072, 768], P('shard'), may hold values from -0.109375 to 0.109375
- query_bias: float32 [768], P('shard'), may hold values from -3 to 3
- value_bias: float32 [768], P('shard'), may hold values from -3 to 3
- out_bias: float32 [768], P('shard'), may hold values from -3 to 3
- attn_gain: float32 [768], P('shard'), may hold values from 0.5 to 1.5
- attn_shift: float32 [768], P('shard'), may hold values from -2 to 2
- up_bias: float32 [3072], P('shard'), may hold values from -3 to 3
- down_bias: float32 [768], P('shard'), may hold values from -3 to 3
- final_gain: float32 [768], P('shard'), may hold values from 0.5 to 1.5
- final_shift: float32 [768], P('shard'), may hold values from -2 to 2
Outputs:
- output: bfloat16 [32, 1024, 768], P(('rep', 'shard'))
- input_grad: bfloat16 [32, 1024, 768], P(('rep', 'shard'))
- grad_query_weight: float32 [768, 768], P('shard')
- grad_key_weight: float32 [768, 768], P('shard')
- grad_value_weight: float32 [768, 768], P('shard')
- grad_out_weight: float32 [768, 768], P('shard')
- grad_up_weight: float32 [768, 3072], P('shard')
- grad_down_weight: float32 [3072, 768], P('shard')
- grad_query_bias: float32 [768], P('shard')
- grad_value_bias: float32 [768], P('shard')
- grad_out_bias: float32 [768], P('shard')
- grad_attn_gain: float32 [768], P('shard')
- grad_attn_shift: float32 [768], P('shard')
- grad_up_bias: float32 [3072], P('shard')
- grad_down_bias: float32 [768], P('shard')
- grad_final_gain: float32 [768], P('shard')
- grad_final_shift: float32 [768], P('shard')
The draws below stay inside these ranges and needn't reach their ends.
Inputs may be any that keep to these rules, and one draw needn't show every extreme that they name: `lengths`: each row sums to 5120 and holds 1024 at least once. `dealing`: each row is a permutation.
All inputs are finite; a program needn't handle non-finite values. No bound on the sum of `drop_flags` on one device may be relied on, other than what follows from the above.
Results may differ from the reference program's by a relative error of at most 0.019.
Values may be sent and summed in bfloat16 or wider, within the bound.
A program may use at most 256 MiB of HBM per device.

```python
import math
import jax
import jax.numpy as jnp
import numpy as np
from jax import lax

D = 768
HEADS = 12
HD = 64
FF = 3072
LEN = 1024
GROUP_SEQS = 8
SEQS = 32
N_REP = 4


def with_ends(values, stream_key, smallest, largest):
    longest = values.shape.index(max(values.shape))
    spots = []
    for shift in (0, 1):
        where = [jax.random.randint(jax.random.fold_in(stream_key, axis), (), 0, length) for axis, length in enumerate(values.shape)]
        where[longest] = (where[longest] + shift) % values.shape[longest]
        spots.append(tuple(where))
    return values.at[spots[0]].set(smallest).at[spots[1]].set(largest)


def steps_of(rng, shape, split, smallest, top_value):
    def one(position, parts):
        heights = jax.random.uniform(jax.random.fold_in(jax.random.fold_in(rng, 6), position), (parts,), jnp.float32, smallest / len(split), top_value / len(split))
        return jnp.repeat(jnp.exp(heights), shape[position] // parts).reshape((-1,) + (1,) * (len(shape) - position - 1))

    factor_of = one(*split[0])
    for cut in split[1:]:
        factor_of = factor_of * one(*cut)
    return factor_of


def profile(count, total, most, lean):
    weights = [(1 << 20) // math.isqrt(standing ** lean) + 1 for standing in range(2, count + 1)]
    surplus, holding = total - most - (count - 1), [1] * (count - 1)
    while surplus > 0:
        candidates = [i for i in range(count - 1) if holding[i] < most]
        whole, remaining = sum([weights[i] for i in candidates]), surplus
        for i in candidates:
            extra = min(most - holding[i], max(1, remaining * weights[i] // whole), surplus)
            holding[i] = holding[i] + extra
            surplus = surplus - extra
    return np.array([most] + holding)


def uneven_parts(rng, count, total, most, lean):
    if count == 2:
        one = jax.random.randint(rng, (), max(1, total - most), min(most, total - 1) + 1)
        return jnp.stack([one, total - one])
    sizes = jnp.asarray(profile(count, total, most, lean), jnp.int32)
    pairs = (count - 1) // 2
    giver, sink = sizes[1:1 + 2 * pairs:2], sizes[2:2 + 2 * pairs:2]
    room = jnp.minimum(giver - 1, most - sink)
    shifted = jax.random.randint(jax.random.fold_in(rng, 1), (pairs,), 0, 1 << 20) % (room + 1)
    sizes = sizes.at[1:1 + 2 * pairs:2].set(giver - shifted).at[2:2 + 2 * pairs:2].set(sink + shifted)
    return sizes[jax.random.permutation(jax.random.fold_in(rng, 2), count)]


def scatter_about(key, extent, spread, limit, cuts=(), held_as=jnp.bfloat16):
    loudness = steps_of(key, extent, cuts, -0.22, 0.18) if cuts else 1.0
    entries = jax.random.normal(key, extent, jnp.float32) * spread * loudness
    return jnp.minimum(jnp.maximum(entries, -limit), limit).astype(held_as)


def setup_inputs(seed: int = 0) -> dict:
    key_list = jax.random.split(jax.random.key(seed), 21)
    return {
        "tokens": scatter_about(key_list[0], (SEQS, LEN, D), 1.0, 6.0, ((0, 32),)),
        "cotangent": scatter_about(key_list[1], (SEQS, LEN, D), 1.0, 6.0, ((0, 32),)),
        "lengths": jax.vmap(lambda own: uneven_parts(own, GROUP_SEQS, 5 * GROUP_SEQS * LEN // 8, LEN, 2))(jax.random.split(key_list[2], N_REP)).reshape((N_REP, GROUP_SEQS)).astype(jnp.int32),
        "dealing": jax.vmap(lambda own: jax.random.permutation(own, GROUP_SEQS))(jax.random.split(key_list[3], N_REP)).reshape((N_REP, GROUP_SEQS)).astype(jnp.int32),
        "drop_flags": with_ends((jax.random.randint(key_list[4], (N_REP, GROUP_SEQS), 0, 5) < 1).astype(jnp.int32), jax.random.fold_in(key_list[4], 1), 0, 1),
        "query_weight": scatter_about(key_list[5], (D, D), (D // 2) ** -0.5, 0.3125, ((0, 8),), jnp.float32),
        "key_weight": scatter_about(key_list[6], (D, D), D ** -0.5, 0.21875, ((0, 8),), jnp.float32),
        "value_weight": scatter_about(key_list[7], (D, D), D ** -0.5, 0.21875, ((0, 8),), jnp.float32),
        "out_weight": scatter_about(key_list[8], (D, D), (D // 16) ** -0.5, 0.875, ((0, 8),), jnp.float32),
        "up_weight": scatter_about(key_list[9], (D, FF), D ** -0.5, 0.21875, ((0, 8),), jnp.float32),
        "down_weight": scatter_about(key_list[10], (FF, D), FF ** -0.5, 0.109375, ((0, 8),), jnp.float32),
        "query_bias": scatter_about(key_list[11], (D,), 0.5, 3.0, ((0, 8),), jnp.float32),
        "value_bias": scatter_about(key_list[12], (D,), 0.5, 3.0, ((0, 8),), jnp.float32),
        "out_bias": scatter_about(key_list[13], (D,), 0.5, 3.0, ((0, 8),), jnp.float32),
        "attn_gain": jnp.clip(1.0 + 0.1 * jax.random.normal(key_list[14], (D,), jnp.float32), 0.5, 1.5),
        "attn_shift": scatter_about(key_list[15], (D,), 0.3, 2.0, ((0, 8),), jnp.float32),
        "up_bias": scatter_about(key_list[16], (FF,), 0.5, 3.0, ((0, 8),), jnp.float32),
        "down_bias": scatter_about(key_list[17], (D,), 0.5, 3.0, ((0, 8),), jnp.float32),
        "final_gain": jnp.clip(1.0 + 0.1 * jax.random.normal(key_list[18], (D,), jnp.float32), 0.5, 1.5),
        "final_shift": scatter_about(key_list[19], (D,), 0.3, 2.0, ((0, 8),), jnp.float32),
    }


@jax.custom_vjp
def low(v):
    return lax.optimization_barrier(v.astype(jnp.bfloat16)).astype(jnp.float32)

@jax.custom_vjp
def low_back(v):
    return v

def low_keep(v):
    return (low(v), None)

def low_pass(kept, grad):
    return (grad,)

def back_keep(v):
    return (v, None)

def back_low(kept, grad):
    return (low(grad),)
low.defvjp(low_keep, low_pass)
low_back.defvjp(back_keep, back_low)

def rounded_both(values):
    return low(low_back(values))

def matmul(left, right):
    return jnp.dot(left, right, precision=lax.Precision.HIGHEST)

def layer_norm(summed, gain, shift):
    center = lax.optimization_barrier(jnp.mean(summed, axis=-1, keepdims=True))
    offset = summed - center
    inverse = lax.rsqrt(lax.optimization_barrier(jnp.mean(offset * offset, axis=-1, keepdims=True)) + 1e-05)
    return offset * inverse * gain + shift

def one_sequence(weights, inputs, length, keeping):
    query_weight, key_weight, value_weight, out_weight, up_weight, down_weight, query_bias, value_bias, out_bias, attn_gain, attn_shift, up_bias, down_bias, final_gain, final_shift = weights
    positions = jnp.arange(LEN)
    queries = rounded_both(matmul(inputs, query_weight) + query_bias).reshape(LEN, HEADS, HD)
    keys_all = rounded_both(matmul(inputs, key_weight)).reshape(LEN, HEADS, HD)
    values_all = rounded_both(matmul(inputs, value_weight) + value_bias).reshape(LEN, HEADS, HD)
    scores = low_back(jnp.einsum('qhd,khd->hqk', queries, keys_all, precision=lax.Precision.HIGHEST)) * (1.0 / math.sqrt(HD))
    key_valid = positions < length
    scores = jnp.where(key_valid[None, None, :], scores, -1e+30)
    peaks = lax.optimization_barrier(jnp.max(scores, axis=-1, keepdims=True))
    expons = jnp.exp(scores - peaks)
    probs = expons / lax.optimization_barrier(jnp.sum(expons, axis=-1, keepdims=True))
    mixing = jnp.einsum('hqk,khd->qhd', low(probs), values_all, precision=lax.Precision.HIGHEST)
    context = rounded_both(mixing.reshape(LEN, D))
    attended = low_back(matmul(context, out_weight) + out_bias)
    first = layer_norm(inputs + attended, attn_gain, attn_shift)
    hidden = low_back(matmul(low(first), up_weight) + up_bias)
    active = low(jax.nn.gelu(hidden, approximate=False))
    branch = low_back(matmul(active, down_weight) + down_bias)
    final = layer_norm(first + branch, final_gain, final_shift)
    row_live = (positions < length) & keeping
    return jnp.where(row_live[:, None], final, inputs)

def reference(tokens, cotangent, lengths, dealing, drop_flags, query_weight, key_weight, value_weight, out_weight, up_weight, down_weight, query_bias, value_bias, out_bias, attn_gain, attn_shift, up_bias, down_bias, final_gain, final_shift):
    slot_ids = jnp.arange(dealing.shape[1], dtype=jnp.int32)
    inverse_order = lax.optimization_barrier(jnp.sum(jnp.where(dealing[:, None, :] == slot_ids[None, :, None], slot_ids[None, None, :], 0), axis=2)).astype(jnp.int32)
    flags_given = jnp.take_along_axis(drop_flags, inverse_order, axis=1).reshape(-1)
    keeping = flags_given == 0
    length_all = lengths.reshape(-1)
    masters = (query_weight, key_weight, value_weight, out_weight, up_weight, down_weight, query_bias, value_bias, out_bias, attn_gain, attn_shift, up_bias, down_bias, final_gain, final_shift)
    inputs_all = tokens.astype(jnp.float32)
    cotan_all = cotangent.astype(jnp.float32)

    def forward(params, inputs):
        lowered = tuple((low(master) for master in params))
        per_sequence = jax.checkpoint(lambda packed: one_sequence(lowered, packed[0], packed[1], packed[2]))
        return lax.map(per_sequence, (inputs, length_all, keeping))
    outputs, pullback = jax.vjp(forward, masters, inputs_all)
    grads, input_grad = pullback(cotan_all)
    return (outputs.astype(jnp.bfloat16), input_grad.astype(jnp.bfloat16), grads[0], grads[1], grads[2], grads[3], grads[4], grads[5], grads[6], grads[7], grads[8], grads[9], grads[10], grads[11], grads[12], grads[13], grads[14])
```

```python
import math

import jax
import jax.numpy as jnp
from jax import lax
from jax.sharding import PartitionSpec as P

D = 768
HEADS = 12
HD = 64
LEN = 1024


def for_sending(value):
    return jax.tree.map(lambda a: a.astype(jnp.bfloat16) if a.dtype == jnp.float32 else a, value)


def layer_stats(summed):
    center = jnp.mean(summed, axis=-1, keepdims=True)
    offset = summed - center
    inverse = lax.rsqrt(jnp.mean(offset * offset, axis=-1, keepdims=True) + 1e-05)
    return (offset * inverse, inverse)


def norm_backward(upstream, normed, inverse, gain):
    scaled = upstream * gain
    return inverse * (
        scaled
        - jnp.mean(scaled, axis=-1, keepdims=True)
        - normed * jnp.mean(scaled * normed, axis=-1, keepdims=True)
    )


def contract(left, right):
    return lax.dot_general(
        left, right, (((0,), (0,)), ((), ())), preferred_element_type=jnp.float32
    )


def through(left, right):
    return lax.dot_general(
        left, right, (((1,), (1,)), ((), ())), preferred_element_type=jnp.float32
    )


def score_block(query_blk, keys_seq, key_valid):
    scores = jnp.einsum("qhd,khd->hqk", query_blk, keys_seq, preferred_element_type=jnp.float32) * (
        1.0 / math.sqrt(HD)
    )
    return jnp.where(key_valid[None, None, :], scores, -1e30)


def attend_forward(queries, keys_seq, values_seq, length):
    key_valid = jnp.arange(LEN) < length

    def per_block(query_blk):
        scores = score_block(query_blk, keys_seq, key_valid)
        peaks = jnp.max(scores, axis=-1, keepdims=True)
        expons = jnp.exp(scores - peaks)
        totals = jnp.sum(expons, axis=-1, keepdims=True)
        probs = (expons / totals).astype(jnp.bfloat16)
        context = jnp.einsum("hqk,khd->qhd", probs, values_seq, preferred_element_type=jnp.float32)
        return (context.astype(jnp.bfloat16), peaks + jnp.log(totals))

    return lax.map(per_block, queries)


def attend_backward(queries, keys_seq, values_seq, dcontext, lse_seq, length):
    key_valid = jnp.arange(LEN) < length

    def per_block(carry, inputs):
        query_blk, dctx_blk, lse_blk = inputs
        scores = score_block(query_blk, keys_seq, key_valid)
        probs = jnp.where(key_valid[None, None, :], jnp.exp(scores - lse_blk), 0.0)
        dprobs = jnp.einsum(
            "qhd,khd->hqk", dctx_blk, values_seq, preferred_element_type=jnp.float32
        )
        deltas = jnp.sum(dprobs * probs, axis=-1, keepdims=True)
        dscores = (probs * (dprobs - deltas) * (1.0 / math.sqrt(HD))).astype(jnp.bfloat16)
        dquery = jnp.einsum(
            "hqk,khd->qhd", dscores, keys_seq, preferred_element_type=jnp.float32
        ).astype(jnp.bfloat16)
        dkeys = carry[0] + jnp.einsum(
            "hqk,qhd->khd", dscores, query_blk, preferred_element_type=jnp.float32
        )
        dvalues = carry[1] + jnp.einsum(
            "hqk,qhd->khd", probs.astype(jnp.bfloat16), dctx_blk, preferred_element_type=jnp.float32
        )
        return ((dkeys, dvalues), dquery)

    zeros_kv = jnp.zeros(keys_seq.shape, jnp.float32)
    (dkeys, dvalues), dquery = lax.scan(
        per_block, (zeros_kv, zeros_kv), (queries, dcontext, lse_seq)
    )
    return (dquery, dkeys.astype(jnp.bfloat16), dvalues.astype(jnp.bfloat16))


def body(
    tokens,
    cotangent,
    lengths,
    dealing,
    drop_flags,
    query_weight,
    key_weight,
    value_weight,
    out_weight,
    up_weight,
    down_weight,
    query_bias,
    value_bias,
    out_bias,
    attn_gain,
    attn_shift,
    up_bias,
    down_bias,
    final_gain,
    final_shift,
):
    masters = (
        query_weight,
        key_weight,
        value_weight,
        out_weight,
        up_weight,
        down_weight,
        query_bias,
        value_bias,
        out_bias,
        attn_gain,
        attn_shift,
        up_bias,
        down_bias,
        final_gain,
        final_shift,
    )
    per_device = tokens.shape[0]
    row_count = per_device * LEN
    block_rows = min(512, LEN)
    group_order = dealing[0]
    local_tokens, local_cotan = tokens, cotangent
    first_slot = lax.axis_index("shard") * per_device
    mine = first_slot + jnp.arange(per_device)
    my_lengths = lax.dynamic_slice_in_dim(lengths[0], first_slot, per_device)
    my_flags = jnp.sum(
        jnp.where(group_order[None, :] == mine[:, None], drop_flags[0][None, :], 0), axis=1
    )
    positions = jnp.arange(LEN)
    row_live = ((positions[None, :] < my_lengths[:, None]) & (my_flags[:, None] == 0)).reshape(
        row_count, 1
    )
    lowered = tuple((master.astype(jnp.bfloat16) for master in masters))
    gathered = jax.tree.map(
        lambda part, own: part.astype(own.dtype),
        lax.all_gather(for_sending(lowered), "shard", axis=0, tiled=True),
        lowered,
    )
    (
        query_full,
        key_full,
        value_full,
        out_full,
        up_full,
        down_full,
        query_add,
        value_add,
        out_add,
        attn_scale,
        attn_add,
        up_add,
        down_add,
        final_scale,
        final_add,
    ) = gathered

    def as_blocks(matrix):
        return matrix.reshape(per_device, LEN // block_rows, block_rows, HEADS, HD)

    def as_sequences(matrix):
        return matrix.reshape(per_device, LEN, HEADS, HD)

    flat_tokens = local_tokens.reshape(row_count, D)
    token_float = flat_tokens.astype(jnp.float32)
    queries = (
        jnp.dot(flat_tokens, query_full, preferred_element_type=jnp.float32)
        + query_add.astype(jnp.float32)
    ).astype(jnp.bfloat16)
    keys_all = jnp.dot(flat_tokens, key_full, preferred_element_type=jnp.float32).astype(
        jnp.bfloat16
    )
    values_all = (
        jnp.dot(flat_tokens, value_full, preferred_element_type=jnp.float32)
        + value_add.astype(jnp.float32)
    ).astype(jnp.bfloat16)
    contexts, lse_all = lax.map(
        lambda packed: attend_forward(packed[0], packed[1], packed[2], packed[3]),
        (as_blocks(queries), as_sequences(keys_all), as_sequences(values_all), my_lengths),
    )
    context = contexts.reshape(row_count, D)
    attended = jnp.dot(context, out_full, preferred_element_type=jnp.float32) + out_add.astype(
        jnp.float32
    )
    normed_one, inverse_one = layer_stats(token_float + attended)
    first = normed_one * attn_scale.astype(jnp.float32) + attn_add.astype(jnp.float32)
    first_low = first.astype(jnp.bfloat16)
    hidden = jnp.dot(first_low, up_full, preferred_element_type=jnp.float32) + up_add.astype(
        jnp.float32
    )
    active = jax.nn.gelu(hidden, approximate=False).astype(jnp.bfloat16)
    branch = jnp.dot(active, down_full, preferred_element_type=jnp.float32) + down_add.astype(
        jnp.float32
    )
    normed_two, inverse_two = layer_stats(first + branch)
    final = normed_two * final_scale.astype(jnp.float32) + final_add.astype(jnp.float32)
    output = jnp.where(row_live, final, token_float).astype(jnp.bfloat16)
    cotan_float = local_cotan.reshape(row_count, D).astype(jnp.float32)
    upstream = jnp.where(row_live, cotan_float, 0.0)
    grad_final_scale = jnp.sum(upstream * normed_two, axis=0)
    grad_final_add = jnp.sum(upstream, axis=0)
    dsum_two = norm_backward(upstream, normed_two, inverse_two, final_scale.astype(jnp.float32))
    dbranch = dsum_two.astype(jnp.bfloat16)
    grad_down_add = jnp.sum(dbranch.astype(jnp.float32), axis=0)
    grad_down = contract(active, dbranch)
    dactive = through(dbranch, down_full)
    slope = 0.5 * (1.0 + lax.erf(hidden * (1.0 / math.sqrt(2.0)))) + hidden * jnp.exp(
        -0.5 * hidden * hidden
    ) * (1.0 / math.sqrt(2.0 * math.pi))
    dhidden = (dactive * slope).astype(jnp.bfloat16)
    grad_up_add = jnp.sum(dhidden.astype(jnp.float32), axis=0)
    grad_up = contract(first_low, dhidden)
    dfirst = dsum_two + through(dhidden, up_full)
    grad_attn_scale = jnp.sum(dfirst * normed_one, axis=0)
    grad_attn_add = jnp.sum(dfirst, axis=0)
    dsum_one = norm_backward(dfirst, normed_one, inverse_one, attn_scale.astype(jnp.float32))
    dattended = dsum_one.astype(jnp.bfloat16)
    grad_out_add = jnp.sum(dattended.astype(jnp.float32), axis=0)
    grad_out = contract(context, dattended)
    dcontext = through(dattended, out_full).astype(jnp.bfloat16)
    dqueries, dkeys, dvalues = lax.map(
        lambda packed: attend_backward(
            packed[0], packed[1], packed[2], packed[3], packed[4], packed[5]
        ),
        (
            as_blocks(queries),
            as_sequences(keys_all),
            as_sequences(values_all),
            as_blocks(dcontext),
            lse_all,
            my_lengths,
        ),
    )
    dqueries = dqueries.reshape(row_count, D)
    dkeys = dkeys.reshape(row_count, D)
    dvalues = dvalues.reshape(row_count, D)
    grad_query = contract(flat_tokens, dqueries)
    grad_key = contract(flat_tokens, dkeys)
    grad_value = contract(flat_tokens, dvalues)
    grad_query_add = jnp.sum(dqueries.astype(jnp.float32), axis=0)
    grad_value_add = jnp.sum(dvalues.astype(jnp.float32), axis=0)
    input_grad = (
        dsum_one
        + through(dqueries, query_full)
        + through(dkeys, key_full)
        + through(dvalues, value_full)
        + jnp.where(row_live, 0.0, cotan_float)
    ).astype(jnp.bfloat16)
    local_grads = (
        grad_query,
        grad_key,
        grad_value,
        grad_out,
        grad_up,
        grad_down,
        grad_query_add,
        grad_value_add,
        grad_out_add,
        grad_attn_scale,
        grad_attn_add,
        grad_up_add,
        grad_down_add,
        grad_final_scale,
        grad_final_add,
    )
    shares = (
        lax.psum_scatter(
            local_grads[0].astype(jnp.bfloat16), "shard", scatter_dimension=0, tiled=True
        ).astype(jnp.float32),
        lax.psum_scatter(
            local_grads[1].astype(jnp.bfloat16), "shard", scatter_dimension=0, tiled=True
        ).astype(jnp.float32),
        lax.psum_scatter(
            local_grads[2].astype(jnp.bfloat16), "shard", scatter_dimension=0, tiled=True
        ).astype(jnp.float32),
        lax.psum_scatter(
            local_grads[3].astype(jnp.bfloat16), "shard", scatter_dimension=0, tiled=True
        ).astype(jnp.float32),
        lax.psum_scatter(
            local_grads[4].astype(jnp.bfloat16), "shard", scatter_dimension=0, tiled=True
        ).astype(jnp.float32),
        lax.psum_scatter(
            local_grads[5].astype(jnp.bfloat16), "shard", scatter_dimension=0, tiled=True
        ).astype(jnp.float32),
        lax.psum_scatter(
            local_grads[6].astype(jnp.bfloat16), "shard", scatter_dimension=0, tiled=True
        ).astype(jnp.float32),
        lax.psum_scatter(
            local_grads[7].astype(jnp.bfloat16), "shard", scatter_dimension=0, tiled=True
        ).astype(jnp.float32),
        lax.psum_scatter(
            local_grads[8].astype(jnp.bfloat16), "shard", scatter_dimension=0, tiled=True
        ).astype(jnp.float32),
        lax.psum_scatter(
            local_grads[9].astype(jnp.bfloat16), "shard", scatter_dimension=0, tiled=True
        ).astype(jnp.float32),
        lax.psum_scatter(
            local_grads[10].astype(jnp.bfloat16), "shard", scatter_dimension=0, tiled=True
        ).astype(jnp.float32),
        lax.psum_scatter(
            local_grads[11].astype(jnp.bfloat16), "shard", scatter_dimension=0, tiled=True
        ).astype(jnp.float32),
        lax.psum_scatter(
            local_grads[12].astype(jnp.bfloat16), "shard", scatter_dimension=0, tiled=True
        ).astype(jnp.float32),
        lax.psum_scatter(
            local_grads[13].astype(jnp.bfloat16), "shard", scatter_dimension=0, tiled=True
        ).astype(jnp.float32),
        lax.psum_scatter(
            local_grads[14].astype(jnp.bfloat16), "shard", scatter_dimension=0, tiled=True
        ).astype(jnp.float32),
    )
    totals = (
        lax.psum(shares[0].astype(jnp.bfloat16), "rep").astype(jnp.float32),
        lax.psum(shares[1].astype(jnp.bfloat16), "rep").astype(jnp.float32),
        lax.psum(shares[2].astype(jnp.bfloat16), "rep").astype(jnp.float32),
        lax.psum(shares[3].astype(jnp.bfloat16), "rep").astype(jnp.float32),
        lax.psum(shares[4].astype(jnp.bfloat16), "rep").astype(jnp.float32),
        lax.psum(shares[5].astype(jnp.bfloat16), "rep").astype(jnp.float32),
        lax.psum(shares[6].astype(jnp.bfloat16), "rep").astype(jnp.float32),
        lax.psum(shares[7].astype(jnp.bfloat16), "rep").astype(jnp.float32),
        lax.psum(shares[8].astype(jnp.bfloat16), "rep").astype(jnp.float32),
        lax.psum(shares[9].astype(jnp.bfloat16), "rep").astype(jnp.float32),
        lax.psum(shares[10].astype(jnp.bfloat16), "rep").astype(jnp.float32),
        lax.psum(shares[11].astype(jnp.bfloat16), "rep").astype(jnp.float32),
        lax.psum(shares[12].astype(jnp.bfloat16), "rep").astype(jnp.float32),
        lax.psum(shares[13].astype(jnp.bfloat16), "rep").astype(jnp.float32),
        lax.psum(shares[14].astype(jnp.bfloat16), "rep").astype(jnp.float32),
    )
    final_out = output.reshape(per_device, LEN, D)
    final_grad = input_grad.reshape(per_device, LEN, D)
    return (
        final_out,
        final_grad,
        totals[0],
        totals[1],
        totals[2],
        totals[3],
        totals[4],
        totals[5],
        totals[6],
        totals[7],
        totals[8],
        totals[9],
        totals[10],
        totals[11],
        totals[12],
        totals[13],
        totals[14],
    )


def solution(mesh):
    placed = (
        P(("rep", "shard"), None, None),
        P(("rep", "shard"), None, None),
        P("rep", None),
        P("rep", None),
        P("rep", None),
        P("shard", None),
        P("shard", None),
        P("shard", None),
        P("shard", None),
        P("shard", None),
        P("shard", None),
        P("shard"),
        P("shard"),
        P("shard"),
        P("shard"),
        P("shard"),
        P("shard"),
        P("shard"),
        P("shard"),
        P("shard"),
    )
    return jax.shard_map(
        body,
        mesh=mesh,
        in_specs=placed,
        out_specs=(
            P(("rep", "shard"), None, None),
            P(("rep", "shard"), None, None),
            P("shard", None),
            P("shard", None),
            P("shard", None),
            P("shard", None),
            P("shard", None),
            P("shard", None),
            P("shard"),
            P("shard"),
            P("shard"),
            P("shard"),
            P("shard"),
            P("shard"),
            P("shard"),
            P("shard"),
            P("shard"),
        ),
        check_vma=False,
    )
```

```python
import functools
import math

import jax
import jax.numpy as jnp
from jax import lax
from jax.experimental import pallas as pl
from jax.experimental.pallas import tpu as pltpu
from jax.sharding import PartitionSpec as P

D = 768
HEADS = 12
HD = 64
LEN = 1024
FF = 3072
SLABS = 8
SROWS = D // SLABS
BF = jnp.bfloat16
F32 = jnp.float32
NN = (((1,), (0,)), ((), ()))
NT = (((1,), (1,)), ((), ()))
TN = (((0,), (0,)), ((), ()))
SMEM = pl.BlockSpec(memory_space=pltpu.SMEM)
ANY = pl.BlockSpec(memory_space=pl.ANY)


def dot(left, right, dims=NN):
    return lax.dot_general(left, right, dims, preferred_element_type=F32)


def sds(*shape, dtype=BF):
    return jax.ShapeDtypeStruct(shape, dtype)


def full(shape):
    return pl.BlockSpec(shape, lambda i: (0,) * len(shape), pipeline_mode=pl.Buffered(1))


def rows(count, width):
    return pl.BlockSpec((count, width), lambda i: (i, 0))


def cost(flops, moved):
    return pl.CostEstimate(flops=int(flops), bytes_accessed=int(moved), transcendentals=0)


def split3(value):
    high = value.astype(BF)
    rest = value - high.astype(F32)
    mid = rest.astype(BF)
    return high, mid, (rest - mid.astype(F32)).astype(BF)


def load_pieces(pieces, parts, me, scratch, sem):
    if len(pieces) == 1:
        copy = pltpu.make_async_copy(pieces[0], scratch, sem)
        copy.start()
        copy.wait()
        return
    for index, piece in enumerate(pieces):
        owner, half = me ^ (index // 2), index % 2
        for source, count, base, stride in parts:
            target = pl.multiple_of(base + owner * stride + half * count, 16)
            pltpu.make_async_copy(
                piece.at[pl.ds(source, count), :], scratch.at[pl.ds(target, count), :], sem
            ).start()
    pltpu.make_async_copy(scratch, scratch, sem).wait()


QKV_PARTS = tuple((48 * j, 48, D * j, 96) for j in range(3))
MID_PARTS = tuple((48 * j, 48, D * j, 96) for j in range(5)) + ((240, 192, 5 * D, 384),)
QKV_ROWS = 3 * D
MID_ROWS = 5 * D + FF
UP0 = D
DOWN0 = 5 * D


def qkv_kernel(meta_ref, x_ref, vec_ref, *refs, count):
    pieces, (q_ref, k_ref, v_ref, w_s, sem) = refs[:count], refs[count:]

    @pl.when(pl.program_id(0) == 0)
    def _():
        load_pieces(pieces, QKV_PARTS, meta_ref[2], w_s, sem)

    x = x_ref[...]
    q_ref[...] = ((dot(x, w_s[0:D, :]) + vec_ref[0:1, :]) * 0.125).astype(BF)
    k_ref[...] = dot(x, w_s[D : 2 * D, :]).astype(BF)
    v_ref[...] = (dot(x, w_s[2 * D : 3 * D, :]) + vec_ref[1:2, :]).astype(BF)


def qkv(meta, x, vec, pieces, R=256):
    return pl.pallas_call(
        functools.partial(qkv_kernel, count=len(pieces)),
        grid=(LEN // R,),
        in_specs=[SMEM, rows(R, D), full(vec.shape)] + [ANY] * len(pieces),
        out_specs=[rows(R, D)] * 3,
        out_shape=[sds(LEN, D)] * 3,
        scratch_shapes=[pltpu.VMEM((QKV_ROWS, D), BF), pltpu.SemaphoreType.DMA],
        cost_estimate=cost(2 * LEN * D * 3 * D, 10e6),
        name="qkv",
    )(meta, x, vec, *pieces)


def input_grad_kernel(meta_ref, da_ref, dq_ref, dk_ref, dv_ref, cot_ref, *refs, count, R):
    pieces, (out_ref, w_s, sem) = refs[:count], refs[count:]
    i = pl.program_id(0)

    @pl.when(i == 0)
    def _():
        load_pieces(pieces, QKV_PARTS, meta_ref[2], w_s, sem)

    total = da_ref[...].astype(F32) + dot(dq_ref[...], w_s[0:D, :], NT)
    total += dot(dk_ref[...], w_s[D : 2 * D, :], NT)
    total += dot(dv_ref[...], w_s[2 * D : 3 * D, :], NT)
    row = lax.broadcasted_iota(jnp.int32, (R, 1), 0) + i * R
    live = (row < meta_ref[0]) & (meta_ref[1] == 0)
    out_ref[...] = jnp.where(live, total, cot_ref[...].astype(F32)).astype(BF)


def input_grad(meta, da, dq, dk, dv, cot, pieces, R=256):
    return pl.pallas_call(
        functools.partial(input_grad_kernel, count=len(pieces), R=R),
        grid=(LEN // R,),
        in_specs=[SMEM] + [rows(R, D)] * 5 + [ANY] * len(pieces),
        out_specs=rows(R, D),
        out_shape=sds(LEN, D),
        scratch_shapes=[pltpu.VMEM((QKV_ROWS, D), BF), pltpu.SemaphoreType.DMA],
        cost_estimate=cost(2 * LEN * D * 3 * D, 13e6),
        name="input_grad",
    )(meta, da, dq, dk, dv, cot, *pieces)


def own_lanes(lane, head):
    return (lane < 64) if head == 0 else (lane >= 64)


def attend_kernel(meta_ref, q_ref, k_ref, v_ref, ctx_ref, aug_ref, *, qb):
    length = meta_ref[0]
    lane = lax.broadcasted_iota(jnp.int32, (LEN, 128), 1)
    row = lax.broadcasted_iota(jnp.int32, (LEN, 128), 0)
    bias = jnp.where(row < length, 0.0, -1e30).astype(BF)
    k = k_ref[...]
    v = v_ref[...]
    one = jnp.ones((), BF)
    zero = jnp.zeros((), BF)
    heads = []
    for h in range(2):
        mine = own_lanes(lane, h)
        spare = 64 if h == 0 else 0
        heads.append(
            (
                jnp.where(mine, k, jnp.where(lane == spare + 3, bias, one)),
                jnp.where(mine, v, one),
                spare,
            )
        )
    lane_q = lax.broadcasted_iota(jnp.int32, (qb, 128), 1)

    @pl.loop(0, LEN // qb)
    def _(i):
        r0 = pl.multiple_of(i * qb, qb)
        q = q_ref[pl.ds(r0, qb), :]
        outs = []
        for h in range(2):
            kh, vh, spare = heads[h]
            qh = jnp.where(own_lanes(lane_q, h), q, jnp.where(lane_q == spare + 3, one, zero))
            s = dot(qh, kh, NT)
            peak = jnp.max(s, axis=1, keepdims=True)
            p = jnp.exp(s - peak).astype(BF)
            o = dot(p, vh)
            total = o[:, 64:65] if h == 0 else o[:, 0:1]
            high, mid, low = split3(-(peak + jnp.log(total)))
            aug_ref[h, pl.ds(r0, qb), :] = jnp.where(
                lane_q == spare,
                high,
                jnp.where(lane_q == spare + 1, mid, jnp.where(lane_q == spare + 2, low, qh)),
            )
            outs.append(o / total)
        ctx_ref[pl.ds(r0, qb), :] = jnp.where(lane_q < 64, outs[0], outs[1]).astype(BF)


def attend(meta, q, k, v, first, count, qb=512):
    wide = pl.BlockSpec((LEN, 128), lambda i: (0, i + first))
    return pl.pallas_call(
        functools.partial(attend_kernel, qb=qb),
        grid=(count,),
        in_specs=[SMEM, wide, wide, wide],
        out_specs=[
            pl.BlockSpec((LEN, 128), lambda i: (0, i)),
            pl.BlockSpec((2, LEN, 128), lambda i: (i, 0, 0)),
        ],
        out_shape=[sds(LEN, 128 * count), sds(2 * count, LEN, 128)],
        cost_estimate=cost(count * 2.4e9, count * 1.5e6),
        name="attend",
    )(meta, q, k, v)


def attend_back_kernel(
    meta_ref, aug_ref, k_ref, v_ref, o_ref, do_ref, dq_ref, dk_ref, dv_ref, sums_ref,
    qa_s, doa_s, dom_s, kt_s, dqt_s, *, kb
):
    length = meta_ref[0]
    one = jnp.ones((), BF)
    zero = jnp.zeros((), BF)
    lane = lax.broadcasted_iota(jnp.int32, (LEN, 128), 1)
    do = do_ref[...]
    product = do.astype(F32) * o_ref[...].astype(F32)
    for h in range(2):
        mine = own_lanes(lane, h)
        spare = 64 if h == 0 else 0
        high, mid, low = split3(
            -jnp.sum(jnp.where(mine, product, 0.0), axis=1, keepdims=True)
        )
        own = jnp.where(mine, do, zero)
        dom_s[h] = own
        doa_s[h] = jnp.where(
            lane == spare,
            high,
            jnp.where(lane == spare + 1, mid, jnp.where(lane == spare + 2, low, own)),
        )
        qa_s[h] = jnp.where(mine, aug_ref[h], zero)
    kt_s[...] = k_ref[...].astype(F32).T.astype(BF)
    dqt_s[...] = jnp.zeros_like(dqt_s)
    sums_ref[...] = jnp.zeros_like(sums_ref)
    lane_k = lax.broadcasted_iota(jnp.int32, (kb, 128), 1)

    @pl.loop(0, LEN // kb)
    def _(i):
        r0 = pl.multiple_of(i * kb, kb)
        row = lax.broadcasted_iota(jnp.int32, (kb, 128), 0) + r0
        bias = jnp.where(row < length, 0.0, -1e30).astype(BF)
        k = k_ref[pl.ds(r0, kb), :]
        v = v_ref[pl.ds(r0, kb), :]
        kt = kt_s[:, pl.ds(r0, kb)]
        dk = dv = None
        for h in range(2):
            mine = own_lanes(lane_k, h)
            spare = 64 if h == 0 else 0
            unit = jnp.where((lane_k >= spare) & (lane_k < spare + 3), one, zero)
            kh = jnp.where(mine, k, jnp.where(lane_k == spare + 3, bias, unit))
            vh = jnp.where(mine, v, unit)
            p = jnp.exp(dot(kh, aug_ref[h], NT))
            dp = dot(vh, doa_s[h], NT)
            ds = (p * dp).astype(BF)
            dvh = dot(p.astype(BF), dom_s[h])
            dkh = dot(ds, qa_s[h])
            dqt_s[64 * h : 64 * h + 64, :] += dot(kt[64 * h : 64 * h + 64, :], ds)
            dk, dv = (dkh, dvh) if h == 0 else (dk + dkh, dv + dvh)
        dv_ref[pl.ds(r0, kb), :] = dv.astype(BF)
        dk_ref[pl.ds(r0, kb), :] = dk.astype(BF)
        sums_ref[1:2, :] += jnp.sum(dv, axis=0, keepdims=True)

    dq = (dqt_s[...] * 0.125).T
    sums_ref[0:1, :] = jnp.sum(dq, axis=0, keepdims=True)
    dq_ref[...] = dq.astype(BF)


def attend_back(meta, aug, k, v, o, do, first, local, count, kb=512):
    wide = pl.BlockSpec((LEN, 128), lambda i: (0, i + first))
    near = pl.BlockSpec((LEN, 128), lambda i: (0, i + local))
    out = pl.BlockSpec((LEN, 128), lambda i: (0, i))
    return pl.pallas_call(
        functools.partial(attend_back_kernel, kb=kb),
        grid=(count,),
        in_specs=[
            SMEM, pl.BlockSpec((2, LEN, 128), lambda i: (i + local, 0, 0)), wide, wide, near, wide
        ],
        out_specs=[out, out, out, pl.BlockSpec((8, 128), lambda i: (0, i))],
        out_shape=[sds(LEN, 128 * count)] * 3 + [sds(8, 128 * count, dtype=F32)],
        scratch_shapes=[pltpu.VMEM((2, LEN, 128), BF)] * 3
        + [pltpu.VMEM((128, LEN), BF), pltpu.VMEM((128, LEN), F32)],
        cost_estimate=cost(count * 3.4e9, count * 2.5e6),
        name="attend_back",
    )(meta, aug, k, v, o, do)


def gelu_parts(u):
    t = 1.0 / (1.0 + (0.3275911 * math.sqrt(0.5)) * jnp.abs(u))
    poly = t * (
        0.127414796
        + t * (-0.142248368 + t * (0.7107068705 + t * (-0.7265760135 + t * 0.5307027145)))
    )
    bell = jnp.exp(-0.5 * (u * u))
    tail = poly * bell
    phi = jnp.where(u >= 0, 1.0 - tail, tail)
    return u * phi, phi + u * bell * (1.0 / math.sqrt(2.0 * math.pi))


def norm(h):
    offset = h - jnp.mean(h, axis=1, keepdims=True)
    inverse = lax.rsqrt(jnp.mean(offset * offset, axis=1, keepdims=True) + 1e-05)
    return offset * inverse, inverse


def norm_back(s, normed, inverse):
    return inverse * (
        s
        - jnp.mean(s, axis=1, keepdims=True)
        - normed * jnp.mean(s * normed, axis=1, keepdims=True)
    )


def mid1_kernel(meta_ref, x_ref, ctxa_ref, ctxb_ref, cot_ref, vec_ref, ub_ref, *refs, count, R):
    pieces = refs[:count]
    (out_ref, fl_ref, act_ref, slope_ref, n1_ref, inv_ref, db_ref, sums_ref,
     acc_s, w_s, sem) = refs[count:]
    i = pl.program_id(0)

    @pl.when(i == 0)
    def _():
        load_pieces(pieces, MID_PARTS, meta_ref[2], w_s, sem)
        sums_ref[...] = jnp.zeros_like(sums_ref)

    x = x_ref[...].astype(F32)
    wide = ctxa_ref.shape[1]
    attended = dot(ctxa_ref[...], w_s[0:wide, :]) + dot(ctxb_ref[...], w_s[wide:D, :])
    n1, inv1 = norm(x + attended + vec_ref[2:3, :])
    first = n1 * vec_ref[3:4, :] + vec_ref[4:5, :]
    fl_ref[...] = first.astype(BF)
    n1_ref[...] = n1.astype(BF)
    inv_ref[...] = jnp.broadcast_to(inv1, (R, 128))
    acc_s[...] = first + vec_ref[5:6, :]

    @pl.loop(0, FF // D)
    def _(c):
        c0 = pl.multiple_of(c * D, D)
        u = dot(fl_ref[...], w_s[pl.ds(UP0 + c0, D), :]) + ub_ref[0:1, pl.ds(c0, D)]
        act, slope = gelu_parts(u)
        act = act.astype(BF)
        act_ref[:, pl.ds(c0, D)] = act
        slope_ref[:, pl.ds(c0, D)] = slope.astype(BF)
        acc_s[...] += dot(act, w_s[pl.ds(DOWN0 + c0, D), :])

    n2, inv2 = norm(acc_s[...])
    gain = vec_ref[6:7, :]
    final = n2 * gain + vec_ref[7:8, :]
    row = lax.broadcasted_iota(jnp.int32, (R, 1), 0) + i * R
    live = (row < meta_ref[0]) & (meta_ref[1] == 0)
    out_ref[...] = jnp.where(live, final, x).astype(BF)
    up = jnp.where(live, cot_ref[...].astype(F32), 0.0)
    db = norm_back(up * gain, n2, inv2).astype(BF)
    db_ref[...] = db
    sums_ref[0:1, :] += jnp.sum(up * n2, axis=0, keepdims=True)
    sums_ref[1:2, :] += jnp.sum(up, axis=0, keepdims=True)
    sums_ref[2:3, :] += jnp.sum(db.astype(F32), axis=0, keepdims=True)


def mid1(meta, x, ctxa, ctxb, cot, vec, ub, pieces, R=256):
    return pl.pallas_call(
        functools.partial(mid1_kernel, count=len(pieces), R=R),
        grid=(LEN // R,),
        in_specs=[
            SMEM, rows(R, D), rows(R, ctxa.shape[1]), rows(R, ctxb.shape[1]), rows(R, D),
            full(vec.shape), full(ub.shape),
        ]
        + [ANY] * len(pieces),
        out_specs=[
            rows(R, D), rows(R, D), rows(R, FF), rows(R, FF), rows(R, D), rows(R, 128),
            rows(R, D), pl.BlockSpec((8, D), lambda i: (0, 0)),
        ],
        out_shape=[
            sds(LEN, D), sds(LEN, D), sds(LEN, FF), sds(LEN, FF), sds(LEN, D),
            sds(LEN, 128, dtype=F32), sds(LEN, D), sds(8, D, dtype=F32),
        ],
        scratch_shapes=[
            pltpu.VMEM((R, D), F32), pltpu.VMEM((MID_ROWS, D), BF), pltpu.SemaphoreType.DMA
        ],
        cost_estimate=cost(16e9, 34e6),
        name="mid1",
    )(meta, x, ctxa, ctxb, cot, vec, ub, *pieces)


def mid2_kernel(meta_ref, db_ref, slope_ref, n1_ref, inv_ref, vec_ref, *refs, count, R):
    pieces = refs[:count]
    dh_ref, da_ref, dctx_ref, sums_ref, ups_ref, acc_s, w_s, sem = refs[count:]

    @pl.when(pl.program_id(0) == 0)
    def _():
        load_pieces(pieces, MID_PARTS, meta_ref[2], w_s, sem)
        sums_ref[...] = jnp.zeros_like(sums_ref)
        ups_ref[...] = jnp.zeros_like(ups_ref)

    acc_s[...] = db_ref[...].astype(F32)

    @pl.loop(0, FF // D)
    def _(c):
        c0 = pl.multiple_of(c * D, D)
        dact = dot(db_ref[...], w_s[pl.ds(DOWN0 + c0, D), :], NT)
        dh = (dact * slope_ref[:, pl.ds(c0, D)].astype(F32)).astype(BF)
        dh_ref[:, pl.ds(c0, D)] = dh
        ups_ref[0:1, pl.ds(c0, D)] += jnp.sum(dh.astype(F32), axis=0, keepdims=True)
        acc_s[...] += dot(dh, w_s[pl.ds(UP0 + c0, D), :], NT)

    df = acc_s[...]
    n1 = n1_ref[...].astype(F32)
    da = norm_back(df * vec_ref[3:4, :], n1, inv_ref[:, 0:1]).astype(BF)
    da_ref[...] = da
    dctx_ref[...] = dot(da, w_s[0:D, :], NT).astype(BF)
    sums_ref[0:1, :] += jnp.sum(df * n1, axis=0, keepdims=True)
    sums_ref[1:2, :] += jnp.sum(df, axis=0, keepdims=True)
    sums_ref[2:3, :] += jnp.sum(da.astype(F32), axis=0, keepdims=True)


def mid2(meta, db, slope, n1, inv, vec, pieces, R=256):
    return pl.pallas_call(
        functools.partial(mid2_kernel, count=len(pieces), R=R),
        grid=(LEN // R,),
        in_specs=[SMEM, rows(R, D), rows(R, FF), rows(R, D), rows(R, 128), full(vec.shape)]
        + [ANY] * len(pieces),
        out_specs=[
            rows(R, FF), rows(R, D), rows(R, D),
            pl.BlockSpec((8, D), lambda i: (0, 0)), pl.BlockSpec((8, FF), lambda i: (0, 0)),
        ],
        out_shape=[
            sds(LEN, FF), sds(LEN, D), sds(LEN, D), sds(8, D, dtype=F32), sds(8, FF, dtype=F32)
        ],
        scratch_shapes=[
            pltpu.VMEM((R, D), F32), pltpu.VMEM((MID_ROWS, D), BF), pltpu.SemaphoreType.DMA
        ],
        cost_estimate=cost(12e9, 30e6),
        name="mid2",
    )(meta, db, slope, n1, inv, vec, *pieces)


def slabs_out(scr, me, send_ref, keep_ref, row0, sem):
    copies = []
    for k in range(SLABS):
        source = scr.at[pl.ds(pl.multiple_of((me ^ k) * SROWS, 16), SROWS), :]
        target = (send_ref if k % 2 else keep_ref).at[k // 2, pl.ds(row0, SROWS), :]
        copies.append(pltpu.make_async_copy(source, target, sem.at[k]))
    return copies


def pairs_kernel(meta_ref, *refs, groups, total):
    count = len(groups)
    send_ref, keep_ref, scr, sem = refs[2 * count :]
    me = meta_ref[2]
    step = 0
    waiting = {}
    for g, blocks in enumerate(groups):
        left_ref, right_ref = refs[2 * g], refs[2 * g + 1]
        width = scr.shape[2]
        for b in range(blocks):
            slot = step % 2
            if step >= 2:
                for copy in waiting[step - 2]:
                    copy.wait()
            scr[slot] = dot(left_ref[...], right_ref[:, width * b : width * (b + 1)], TN).astype(BF)
            waiting[step] = slabs_out(
                scr.at[slot], me, send_ref, keep_ref, step * SROWS, sem.at[slot]
            )
            for copy in waiting[step]:
                copy.start()
            step += 1
    for late in (total - 2, total - 1):
        if late >= 0:
            for copy in waiting[late]:
                copy.wait()


def pair_grads(meta, pairs, width):
    groups = tuple(right.shape[1] // width for _, right in pairs)
    total = sum(groups)
    flat = [a for pair in pairs for a in pair]
    vm = pl.BlockSpec(memory_space=pltpu.VMEM)
    return pl.pallas_call(
        functools.partial(pairs_kernel, groups=groups, total=total),
        in_specs=[SMEM] + [vm] * len(flat),
        out_specs=[ANY, ANY],
        out_shape=[sds(4, total * SROWS, width)] * 2,
        scratch_shapes=[pltpu.VMEM((2, D, width), BF), pltpu.SemaphoreType.DMA((2, SLABS))],
        cost_estimate=cost(2 * LEN * D * width * total * 1.2, 15e6),
        name="pair_grads",
    )(meta, *flat)


def down_kernel(meta_ref, act_ref, db_ref, send_ref, keep_ref):
    i = pl.program_id(0)
    value = dot(act_ref[...], db_ref[...], TN).astype(BF)

    @pl.when(i < 4)
    def _():
        send_ref[0] = value

    @pl.when(i >= 4)
    def _():
        keep_ref[0] = value


def down_grads(meta, act, db):
    def owner(i, m):
        k = jnp.where(i < 4, 2 * i + 1, 2 * (i - 4))
        return m[2] ^ k

    return pl.pallas_call(
        down_kernel,
        grid_spec=pltpu.PrefetchScalarGridSpec(
            num_scalar_prefetch=1,
            grid=(SLABS,),
            in_specs=[
                pl.BlockSpec((LEN, FF // SLABS), lambda i, m: (0, owner(i, m))),
                pl.BlockSpec((LEN, D), lambda i, m: (0, 0), pipeline_mode=pl.Buffered(1)),
            ],
            out_specs=[
                pl.BlockSpec((1, FF // SLABS, D), lambda i, m: (jnp.minimum(i, 3), 0, 0)),
                pl.BlockSpec((1, FF // SLABS, D), lambda i, m: (jnp.maximum(i - 4, 0), 0, 0)),
            ],
        ),
        out_shape=[sds(4, FF // SLABS, D)] * 2,
        cost_estimate=cost(2 * LEN * FF * D * 1.2, 13e6),
        name="down_grads",
    )(meta, act, db)


def swap(value, axis, bit, size):
    return lax.ppermute(value, axis, [(i, i ^ bit) for i in range(size)])


def gather_halves(halves):
    pieces = [None] * 16
    held = [{0: halves[0]}, {0: halves[1]}]
    for stage in range(3):
        for h, order in enumerate(((2, 4, 1), (4, 2, 1))):
            bit = order[stage]
            held[h].update({k ^ bit: swap(v, "shard", bit, 8) for k, v in list(held[h].items())})
    for h in range(2):
        for k, v in held[h].items():
            pieces[2 * k + h] = v
    return pieces


def add(*terms):
    return sum(t.astype(F32) for t in terms).astype(BF)


def reduce_slabs(send, keep):
    got = swap(send, "shard", 1, 8)
    half = send.shape[1] // 2
    ends = []
    for cut, first, second, out, stay in (
        (slice(0, half), 2, 4, (1, 3), (0, 2)),
        (slice(half, None), 4, 2, (2, 3), (0, 1)),
    ):
        away = [add(keep[p, cut], got[p, cut]) for p in out]
        back = swap(jnp.stack(away), "shard", first, 8)
        far = add(keep[stay[1], cut], got[stay[1], cut], back[1])
        last = swap(far, "shard", second, 8)
        ends.append(add(keep[0, cut], got[0, cut], back[0], last))
    return jnp.concatenate(ends)


def reduce_rep(value, place):
    quarter = value.shape[0] // 4
    parts = value.reshape(4, quarter, value.shape[1])
    mine = lax.dynamic_index_in_dim(parts, place, 0, False)
    terms = [mine]
    for k in (1, 2, 3):
        part = lax.dynamic_index_in_dim(parts, place ^ k, 0, False)
        terms.append(swap(part, "rep", k, 4))
    total = add(*terms)
    out = jnp.zeros(parts.shape, F32)
    out = lax.dynamic_update_index_in_dim(out, total.astype(F32), place, 0)
    for k in (1, 2, 3):
        out = lax.dynamic_update_index_in_dim(
            out, swap(total, "rep", k, 4).astype(F32), place ^ k, 0
        )
    return out.reshape(value.shape)


def whole_slabs(send, keep):
    return jnp.stack([keep, send], axis=1).reshape((SLABS,) + send.shape[1:])


def reduce_any(matrix):
    share = lax.psum_scatter(matrix, "shard", scatter_dimension=0, tiled=True)
    return lax.psum(share, "rep").astype(F32)


def body(n_shard, n_rep, tokens, cotangent, lengths, dealing, drop_flags, *masters):
    matrices = [m.astype(BF) for m in masters[:6]]
    vectors = [m.astype(BF) for m in masters[6:]]
    permuted = n_shard == 8 and n_rep == 4
    position = lax.axis_index("shard")
    me = position if permuted else jnp.zeros((), jnp.int32)
    place = lax.axis_index("rep")
    length = lax.dynamic_index_in_dim(lengths[0], position, 0, False)
    flag = jnp.sum(jnp.where(dealing[0] == position, drop_flags[0], 0))
    meta = jnp.stack([length, flag, me]).astype(jnp.int32)
    x = tokens.reshape(LEN, D)
    cot = cotangent.reshape(LEN, D)

    names = vectors[:5] + vectors[6:9]
    width = D // n_shard
    small = jnp.concatenate([v[None] for v in names] + [vectors[5].reshape(4, width)])
    wq, wk, wv, wo, wu, wd = matrices
    if permuted:
        held = small[None]
        for bit in (1, 2, 4):
            held = jnp.concatenate([held, swap(held, "shard", bit, 8)])
        every = jnp.take(held, jnp.arange(8, dtype=jnp.int32) ^ position, axis=0)
        ups = [wu[:, D * j : D * (j + 1)] for j in range(4)]
        cuts = (slice(0, 48), slice(48, 96))
        near = gather_halves(
            [jnp.concatenate([m[c] for m in (wq, wk, wv)]) for c in cuts]
        )
        down_cuts = (slice(0, 192), slice(192, 384))
        far_halves = [
            jnp.concatenate([m[c] for m in [wo] + ups] + [wd[c2]])
            for c, c2 in zip(cuts, down_cuts)
        ]
        far_halves[0], far_halves[1], near = lax.optimization_barrier(
            (far_halves[0], far_halves[1], near)
        )
        far = gather_halves(far_halves)
    else:
        every = lax.all_gather(small, "shard", axis=0)
        whole = [lax.all_gather(m, "shard", axis=0, tiled=True) for m in matrices]
        near = [jnp.concatenate(whole[:3])]
        far = [
            jnp.concatenate(
                [whole[3]] + [whole[4][:, D * j : D * (j + 1)] for j in range(4)] + [whole[5]]
            )
        ]
    every = every.astype(F32)
    vec = every[:, :8].transpose(1, 0, 2).reshape(8, D)
    ub = every[:, 8:].reshape(1, FF)
    ub = jnp.broadcast_to(ub, (8, FF))

    q, k, v = qkv(meta, x, vec, near)
    ctxa, auga = attend(meta, q, k, v, 0, 4)
    ctxb, augb = attend(meta, q, k, v, 4, 2)
    output, first, act, slope, n1, inv, db, sums1 = mid1(meta, x, ctxa, ctxb, cot, vec, ub, far)
    down = down_grads(meta, act, db)
    dh, da, dctx, sums2, sums_up = mid2(meta, db, slope, n1, inv, vec, far)
    ctx = jnp.concatenate([ctxa, ctxb], axis=1)
    upout = pair_grads(meta, ((first, dh), (ctx, da)), D)
    dqa, dka, dva, sums_a = attend_back(meta, auga, k, v, ctxa, dctx, 0, 0, 4)
    qkva = pair_grads(meta, ((x, dqa), (x, dka), (x, dva)), 512)
    dqb, dkb, dvb, sums_b = attend_back(meta, augb, k, v, ctxb, dctx, 4, 0, 2)
    qkvb = pair_grads(meta, ((x, dqb), (x, dkb), (x, dvb)), 256)
    dq, dk, dv = (
        jnp.concatenate(p, axis=1) for p in ((dqa, dqb), (dka, dkb), (dva, dvb))
    )
    grad_x = input_grad(meta, da, dq, dk, dv, cot, near)

    sums_ab = jnp.concatenate([sums_a[:2], sums_b[:2]], axis=1)
    sums = jnp.concatenate(
        [
            sums_ab, sums2[2:3], sums2[0:2], sums1[2:3], sums1[0:2],
            sums_up[0].reshape(4, D),
        ]
    )
    if permuted:
        for bit in (1, 2, 4):
            sums = sums + swap(sums, "shard", bit, 8)
        for bit in (1, 2):
            sums = sums + swap(sums, "rep", bit, 4)
    else:
        sums = lax.psum(sums, ("rep", "shard"))
    grads_v = [
        lax.dynamic_slice_in_dim(sums[r], position * width, width) for r in range(8)
    ]
    grad_ub = lax.dynamic_slice_in_dim(
        sums[8:].reshape(FF), position * (FF // n_shard), FF // n_shard
    )

    if permuted:
        grad_down = reduce_rep(reduce_slabs(*down), place)
        g_uo = reduce_rep(reduce_slabs(*upout), place)
        g_a = reduce_rep(reduce_slabs(*qkva), place)
        g_b = reduce_rep(reduce_slabs(*qkvb), place)
        grad_up = jnp.concatenate([g_uo[96 * j : 96 * (j + 1)] for j in range(4)], axis=1)
        grad_out = g_uo[384:]
        grad_qkv = [
            jnp.concatenate([g[96 * j : 96 * (j + 1)] for g in (g_a, g_b)], axis=1)
            for j in range(3)
        ]
    else:
        def rebuild(slabs, j):
            return slabs[:, SROWS * j : SROWS * (j + 1)].reshape(D, slabs.shape[2])

        grad_down = reduce_any(whole_slabs(*down).reshape(FF, D))
        g_uo, g_a, g_b = (whole_slabs(*p) for p in (upout, qkva, qkvb))
        grad_up = reduce_any(jnp.concatenate([rebuild(g_uo, j) for j in range(4)], axis=1))
        grad_out = reduce_any(rebuild(g_uo, 4))
        grad_qkv = [
            reduce_any(jnp.concatenate([rebuild(g, j) for g in (g_a, g_b)], axis=1))
            for j in range(3)
        ]
    return (
        output.reshape(tokens.shape),
        grad_x.reshape(tokens.shape),
        grad_qkv[0],
        grad_qkv[1],
        grad_qkv[2],
        grad_out,
        grad_up,
        grad_down,
        grads_v[0],
        grads_v[1],
        grads_v[2],
        grads_v[3],
        grads_v[4],
        grad_ub,
        grads_v[5],
        grads_v[6],
        grads_v[7],
    )


def solution(mesh):
    tokens = P(("rep", "shard"), None, None)
    table = P("rep", None)
    matrix = P("shard", None)
    vector = P("shard")
    return jax.shard_map(
        functools.partial(body, mesh.shape["shard"], mesh.shape["rep"]),
        mesh=mesh,
        in_specs=(tokens, tokens) + (table,) * 3 + (matrix,) * 6 + (vector,) * 9,
        out_specs=(tokens, tokens) + (matrix,) * 6 + (vector,) * 9,
        check_vma=False,
    )
```

```python
import functools
import math

import jax
import jax.numpy as jnp
from jax import lax
from jax.experimental import pallas as pl
from jax.experimental.pallas import tpu as pltpu
from jax.sharding import PartitionSpec as P

D = 768
HEADS = 12
HD = 64
LEN = 1024
FF = 3072
SLABS = 8
SROWS = D // SLABS
BF = jnp.bfloat16
F32 = jnp.float32
NN = (((1,), (0,)), ((), ()))
NT = (((1,), (1,)), ((), ()))
TN = (((0,), (0,)), ((), ()))
SMEM = pl.BlockSpec(memory_space=pltpu.SMEM)
ANY = pl.BlockSpec(memory_space=pl.ANY)


def dot(left, right, dims=NN):
    return lax.dot_general(left, right, dims, preferred_element_type=F32)


def sds(*shape, dtype=BF):
    return jax.ShapeDtypeStruct(shape, dtype)


def full(shape):
    return pl.BlockSpec(shape, lambda i: (0,) * len(shape), pipeline_mode=pl.Buffered(1))


def rows(count, width):
    return pl.BlockSpec((count, width), lambda i: (i, 0))


def cost(flops, moved):
    return pl.CostEstimate(flops=int(flops), bytes_accessed=int(moved), transcendentals=0)


def split3(value):
    high = value.astype(BF)
    rest = value - high.astype(F32)
    mid = rest.astype(BF)
    return high, mid, (rest - mid.astype(F32)).astype(BF)


def load_pieces(pieces, parts, me, scratch, sem):
    if len(pieces) == 1:
        copy = pltpu.make_async_copy(pieces[0], scratch, sem)
        copy.start()
        copy.wait()
        return
    for index, piece in enumerate(pieces):
        owner, half = me ^ (index // 2), index % 2
        for source, count, base, stride in parts:
            target = pl.multiple_of(base + owner * stride + half * count, 16)
            pltpu.make_async_copy(
                piece.at[pl.ds(source, count), :], scratch.at[pl.ds(target, count), :], sem
            ).start()
    pltpu.make_async_copy(scratch, scratch, sem).wait()


QKV_PARTS = tuple((48 * j, 48, D * j, 96) for j in range(3))
MID_PARTS = tuple((48 * j, 48, D * j, 96) for j in range(5)) + ((240, 192, 5 * D, 384),)
QKV_ROWS = 3 * D
MID_ROWS = 5 * D + FF
UP0 = D
DOWN0 = 5 * D


def qkv_kernel(meta_ref, x_ref, vec_ref, *refs, count):
    pieces, (q_ref, k_ref, v_ref, w_s, sem) = refs[:count], refs[count:]

    @pl.when(pl.program_id(0) == 0)
    def _():
        load_pieces(pieces, QKV_PARTS, meta_ref[2], w_s, sem)

    x = x_ref[...]
    q_ref[...] = ((dot(x, w_s[0:D, :]) + vec_ref[0:1, :]) * 0.125).astype(BF)
    k_ref[...] = dot(x, w_s[D : 2 * D, :]).astype(BF)
    v_ref[...] = (dot(x, w_s[2 * D : 3 * D, :]) + vec_ref[1:2, :]).astype(BF)


def qkv(meta, x, vec, pieces, R=256):
    return pl.pallas_call(
        functools.partial(qkv_kernel, count=len(pieces)),
        grid=(LEN // R,),
        in_specs=[SMEM, rows(R, D), full(vec.shape)] + [ANY] * len(pieces),
        out_specs=[rows(R, D)] * 3,
        out_shape=[sds(LEN, D)] * 3,
        scratch_shapes=[pltpu.VMEM((QKV_ROWS, D), BF), pltpu.SemaphoreType.DMA],
        cost_estimate=cost(2 * LEN * D * 3 * D, 10e6),
        name="qkv",
    )(meta, x, vec, *pieces)


def input_grad_kernel(meta_ref, da_ref, dq_ref, dk_ref, dv_ref, cot_ref, *refs, count, R):
    pieces, (out_ref, w_s, sem) = refs[:count], refs[count:]
    i = pl.program_id(0)

    @pl.when(i == 0)
    def _():
        load_pieces(pieces, QKV_PARTS, meta_ref[2], w_s, sem)

    total = da_ref[...].astype(F32) + dot(dq_ref[...], w_s[0:D, :], NT)
    total += dot(dk_ref[...], w_s[D : 2 * D, :], NT)
    total += dot(dv_ref[...], w_s[2 * D : 3 * D, :], NT)
    row = lax.broadcasted_iota(jnp.int32, (R, 1), 0) + i * R
    live = (row < meta_ref[0]) & (meta_ref[1] == 0)
    out_ref[...] = jnp.where(live, total, cot_ref[...].astype(F32)).astype(BF)


def input_grad(meta, da, dq, dk, dv, cot, pieces, R=256):
    return pl.pallas_call(
        functools.partial(input_grad_kernel, count=len(pieces), R=R),
        grid=(LEN // R,),
        in_specs=[SMEM] + [rows(R, D)] * 5 + [ANY] * len(pieces),
        out_specs=rows(R, D),
        out_shape=sds(LEN, D),
        scratch_shapes=[pltpu.VMEM((QKV_ROWS, D), BF), pltpu.SemaphoreType.DMA],
        cost_estimate=cost(2 * LEN * D * 3 * D, 13e6),
        name="input_grad",
    )(meta, da, dq, dk, dv, cot, *pieces)


def own_lanes(lane, head):
    return (lane < 64) if head == 0 else (lane >= 64)


def attend_kernel(meta_ref, q_ref, k_ref, v_ref, *refs, qb):
    ctx_ref, aug_ref = refs[-2:]
    length = meta_ref[0]
    lane = lax.broadcasted_iota(jnp.int32, (LEN, 128), 1)
    row = lax.broadcasted_iota(jnp.int32, (LEN, 128), 0)
    bias = jnp.where(row < length, 0.0, -1e30).astype(BF)
    k = k_ref[...]
    v = v_ref[...]
    one = jnp.ones((), BF)
    zero = jnp.zeros((), BF)
    heads = []
    for h in range(2):
        mine = own_lanes(lane, h)
        spare = 64 if h == 0 else 0
        heads.append(
            (
                jnp.where(mine, k, jnp.where(lane == spare + 3, bias, one)),
                jnp.where(mine, v, one),
                spare,
            )
        )
    lane_q = lax.broadcasted_iota(jnp.int32, (qb, 128), 1)

    @pl.loop(0, LEN // qb)
    def _(i):
        r0 = pl.multiple_of(i * qb, qb)
        q = q_ref[pl.ds(r0, qb), :]
        outs = []
        for h in range(2):
            kh, vh, spare = heads[h]
            qh = jnp.where(own_lanes(lane_q, h), q, jnp.where(lane_q == spare + 3, one, zero))
            s = dot(qh, kh, NT)
            peak = jnp.max(s, axis=1, keepdims=True)
            p = jnp.exp(s - peak).astype(BF)
            o = dot(p, vh)
            total = o[:, 64:65] if h == 0 else o[:, 0:1]
            high, mid, low = split3(-(peak + jnp.log(total)))
            aug_ref[h, pl.ds(r0, qb), :] = jnp.where(
                lane_q == spare,
                high,
                jnp.where(lane_q == spare + 1, mid, jnp.where(lane_q == spare + 2, low, qh)),
            )
            outs.append(o / total)
        ctx_ref[pl.ds(r0, qb), :] = jnp.where(lane_q < 64, outs[0], outs[1]).astype(BF)


def attend(meta, q, k, v, held, first, count, qb=512):
    wide = pl.BlockSpec((LEN, 128), lambda i: (0, i + first))
    return pl.pallas_call(
        functools.partial(attend_kernel, qb=qb),
        grid=(count,),
        in_specs=[SMEM, wide, wide, wide] + [ANY] * len(held),
        out_specs=[wide, pl.BlockSpec((2, LEN, 128), lambda i: (i + first, 0, 0))],
        out_shape=[sds(LEN, D), sds(HEADS, LEN, 128)],
        input_output_aliases={4 + j: j for j in range(len(held))},
        cost_estimate=cost(count * 2.4e9, count * 1.5e6),
        name="attend",
    )(meta, q, k, v, *held)


def attend_back_kernel(meta_ref, aug_ref, k_ref, v_ref, o_ref, do_ref, old_ref, *refs, kb):
    dq_ref, dk_ref, dv_ref, sums_ref, qa_s, doa_s, dom_s, kt_s, dqt_s = refs[-9:]
    length = meta_ref[0]
    one = jnp.ones((), BF)
    zero = jnp.zeros((), BF)
    lane = lax.broadcasted_iota(jnp.int32, (LEN, 128), 1)
    do = do_ref[...]
    product = do.astype(F32) * o_ref[...].astype(F32)
    for h in range(2):
        mine = own_lanes(lane, h)
        spare = 64 if h == 0 else 0
        high, mid, low = split3(
            -jnp.sum(jnp.where(mine, product, 0.0), axis=1, keepdims=True)
        )
        own = jnp.where(mine, do, zero)
        dom_s[h] = own
        doa_s[h] = jnp.where(
            lane == spare,
            high,
            jnp.where(lane == spare + 1, mid, jnp.where(lane == spare + 2, low, own)),
        )
        qa_s[h] = jnp.where(mine, aug_ref[h], zero)
    kt_s[...] = k_ref[...].astype(F32).T.astype(BF)
    dqt_s[...] = jnp.zeros_like(dqt_s)
    sums_ref[...] = old_ref[...]
    lane_k = lax.broadcasted_iota(jnp.int32, (kb, 128), 1)

    @pl.loop(0, LEN // kb)
    def _(i):
        r0 = pl.multiple_of(i * kb, kb)
        row = lax.broadcasted_iota(jnp.int32, (kb, 128), 0) + r0
        bias = jnp.where(row < length, 0.0, -1e30).astype(BF)
        k = k_ref[pl.ds(r0, kb), :]
        v = v_ref[pl.ds(r0, kb), :]
        kt = kt_s[:, pl.ds(r0, kb)]
        dk = dv = None
        for h in range(2):
            mine = own_lanes(lane_k, h)
            spare = 64 if h == 0 else 0
            unit = jnp.where((lane_k >= spare) & (lane_k < spare + 3), one, zero)
            kh = jnp.where(mine, k, jnp.where(lane_k == spare + 3, bias, unit))
            vh = jnp.where(mine, v, unit)
            p = jnp.exp(dot(kh, aug_ref[h], NT))
            dp = dot(vh, doa_s[h], NT)
            ds = (p * dp).astype(BF)
            dvh = dot(p.astype(BF), dom_s[h])
            dkh = dot(ds, qa_s[h])
            dqt_s[64 * h : 64 * h + 64, :] += dot(kt[64 * h : 64 * h + 64, :], ds)
            dk, dv = (dkh, dvh) if h == 0 else (dk + dkh, dv + dvh)
        dv_ref[pl.ds(r0, kb), :] = dv.astype(BF)
        dk_ref[pl.ds(r0, kb), :] = dk.astype(BF)
        sums_ref[1:2, :] += jnp.sum(dv, axis=0, keepdims=True)

    dq = (dqt_s[...] * 0.125).T
    sums_ref[0:1, :] = jnp.sum(dq, axis=0, keepdims=True)
    dq_ref[...] = dq.astype(BF)


def attend_back(meta, aug, k, v, o, do, sums, held, first, count, kb=512):
    wide = pl.BlockSpec((LEN, 128), lambda i: (0, i + first))
    tall = pl.BlockSpec((16, 128), lambda i: (0, i + first))
    aliases = {6: 3}
    aliases.update({7 + j: j for j in range(len(held))})
    return pl.pallas_call(
        functools.partial(attend_back_kernel, kb=kb),
        grid=(count,),
        in_specs=[SMEM, pl.BlockSpec((2, LEN, 128), lambda i: (i + first, 0, 0))]
        + [wide] * 4
        + [tall]
        + [ANY] * len(held),
        out_specs=[wide, wide, wide, tall],
        out_shape=[sds(LEN, D)] * 3 + [sds(16, D, dtype=F32)],
        scratch_shapes=[pltpu.VMEM((2, LEN, 128), BF)] * 3
        + [pltpu.VMEM((128, LEN), BF), pltpu.VMEM((128, LEN), F32)],
        input_output_aliases=aliases,
        cost_estimate=cost(count * 3.4e9, count * 2.5e6),
        name="attend_back",
    )(meta, aug, k, v, o, do, sums, *held)


def gelu_parts(u):
    t = 1.0 / (1.0 + (0.3275911 * math.sqrt(0.5)) * jnp.abs(u))
    poly = t * (
        0.127414796
        + t * (-0.142248368 + t * (0.7107068705 + t * (-0.7265760135 + t * 0.5307027145)))
    )
    bell = jnp.exp(-0.5 * (u * u))
    tail = poly * bell
    phi = jnp.where(u >= 0, 1.0 - tail, tail)
    return u * phi, phi + u * bell * (1.0 / math.sqrt(2.0 * math.pi))


def norm(h):
    offset = h - jnp.mean(h, axis=1, keepdims=True)
    inverse = lax.rsqrt(jnp.mean(offset * offset, axis=1, keepdims=True) + 1e-05)
    return offset * inverse, inverse


def norm_back(s, normed, inverse):
    return inverse * (
        s
        - jnp.mean(s, axis=1, keepdims=True)
        - normed * jnp.mean(s * normed, axis=1, keepdims=True)
    )


def mid1_kernel(meta_ref, x_ref, ctx_ref, cot_ref, vec_ref, ub_ref, *refs, count, R):
    pieces = refs[:count]
    (out_ref, fl_ref, act_ref, slope_ref, n1_ref, inv_ref, db_ref, sums_ref,
     acc_s, w_s, sem) = refs[count:]
    i = pl.program_id(0)

    @pl.when(i == 0)
    def _():
        load_pieces(pieces, MID_PARTS, meta_ref[2], w_s, sem)
        sums_ref[...] = jnp.zeros_like(sums_ref)

    x = x_ref[...].astype(F32)
    attended = dot(ctx_ref[...], w_s[0:D, :])
    n1, inv1 = norm(x + attended + vec_ref[2:3, :])
    first = n1 * vec_ref[3:4, :] + vec_ref[4:5, :]
    fl_ref[...] = first.astype(BF)
    n1_ref[...] = n1.astype(BF)
    inv_ref[...] = jnp.broadcast_to(inv1, (R, 128))
    acc_s[...] = first + vec_ref[5:6, :]

    @pl.loop(0, FF // D)
    def _(c):
        c0 = pl.multiple_of(c * D, D)
        u = dot(fl_ref[...], w_s[pl.ds(UP0 + c0, D), :]) + ub_ref[0:1, pl.ds(c0, D)]
        act, slope = gelu_parts(u)
        act = act.astype(BF)
        act_ref[:, pl.ds(c0, D)] = act
        slope_ref[:, pl.ds(c0, D)] = slope.astype(BF)
        acc_s[...] += dot(act, w_s[pl.ds(DOWN0 + c0, D), :])

    n2, inv2 = norm(acc_s[...])
    gain = vec_ref[6:7, :]
    final = n2 * gain + vec_ref[7:8, :]
    row = lax.broadcasted_iota(jnp.int32, (R, 1), 0) + i * R
    live = (row < meta_ref[0]) & (meta_ref[1] == 0)
    out_ref[...] = jnp.where(live, final, x).astype(BF)
    up = jnp.where(live, cot_ref[...].astype(F32), 0.0)
    db = norm_back(up * gain, n2, inv2).astype(BF)
    db_ref[...] = db
    sums_ref[5:6, :] += jnp.sum(db.astype(F32), axis=0, keepdims=True)
    sums_ref[6:7, :] += jnp.sum(up * n2, axis=0, keepdims=True)
    sums_ref[7:8, :] += jnp.sum(up, axis=0, keepdims=True)


def mid1(meta, x, ctx, cot, vec, ub, pieces, R=256):
    return pl.pallas_call(
        functools.partial(mid1_kernel, count=len(pieces), R=R),
        grid=(LEN // R,),
        in_specs=[
            SMEM, rows(R, D), rows(R, D), rows(R, D),
            full(vec.shape), full(ub.shape),
        ]
        + [ANY] * len(pieces),
        out_specs=[
            rows(R, D), rows(R, D), rows(R, FF), rows(R, FF), rows(R, D), rows(R, 128),
            rows(R, D), pl.BlockSpec((8, D), lambda i: (0, 0)),
        ],
        out_shape=[
            sds(LEN, D), sds(LEN, D), sds(LEN, FF), sds(LEN, FF), sds(LEN, D),
            sds(LEN, 128, dtype=F32), sds(LEN, D), sds(8, D, dtype=F32),
        ],
        scratch_shapes=[
            pltpu.VMEM((R, D), F32), pltpu.VMEM((MID_ROWS, D), BF), pltpu.SemaphoreType.DMA
        ],
        cost_estimate=cost(16e9, 34e6),
        name="mid1",
    )(meta, x, ctx, cot, vec, ub, *pieces)


def mid2_kernel(meta_ref, db_ref, slope_ref, n1_ref, inv_ref, vec_ref, old_ref, *refs, count, R):
    pieces = refs[:count]
    dh_ref, da_ref, dctx_ref, sums_ref, acc_s, w_s, sem = refs[count:]

    @pl.when(pl.program_id(0) == 0)
    def _():
        load_pieces(pieces, MID_PARTS, meta_ref[2], w_s, sem)
        sums_ref[0:8, :] = old_ref[...]
        sums_ref[8:16, :] = jnp.zeros_like(old_ref)

    acc_s[...] = db_ref[...].astype(F32)

    @pl.loop(0, FF // D)
    def _(c):
        c0 = pl.multiple_of(c * D, D)
        dact = dot(db_ref[...], w_s[pl.ds(DOWN0 + c0, D), :], NT)
        dh = (dact * slope_ref[:, pl.ds(c0, D)].astype(F32)).astype(BF)
        dh_ref[:, pl.ds(c0, D)] = dh
        sums_ref[pl.ds(8 + c, 1), :] += jnp.sum(dh.astype(F32), axis=0, keepdims=True)
        acc_s[...] += dot(dh, w_s[pl.ds(UP0 + c0, D), :], NT)

    df = acc_s[...]
    n1 = n1_ref[...].astype(F32)
    da = norm_back(df * vec_ref[3:4, :], n1, inv_ref[:, 0:1]).astype(BF)
    da_ref[...] = da
    dctx_ref[...] = dot(da, w_s[0:D, :], NT).astype(BF)
    sums_ref[2:3, :] += jnp.sum(da.astype(F32), axis=0, keepdims=True)
    sums_ref[3:4, :] += jnp.sum(df * n1, axis=0, keepdims=True)
    sums_ref[4:5, :] += jnp.sum(df, axis=0, keepdims=True)


def mid2(meta, db, slope, n1, inv, vec, sums, pieces, R=256):
    return pl.pallas_call(
        functools.partial(mid2_kernel, count=len(pieces), R=R),
        grid=(LEN // R,),
        in_specs=[SMEM, rows(R, D), rows(R, FF), rows(R, D), rows(R, 128), full(vec.shape), full((8, D))]
        + [ANY] * len(pieces),
        out_specs=[
            rows(R, FF), rows(R, D), rows(R, D), pl.BlockSpec((16, D), lambda i: (0, 0)),
        ],
        out_shape=[
            sds(LEN, FF), sds(LEN, D), sds(LEN, D), sds(16, D, dtype=F32)
        ],
        scratch_shapes=[
            pltpu.VMEM((R, D), F32), pltpu.VMEM((MID_ROWS, D), BF), pltpu.SemaphoreType.DMA
        ],
        cost_estimate=cost(12e9, 30e6),
        name="mid2",
    )(meta, db, slope, n1, inv, vec, sums, *pieces)


def slabs_out(scr, me, send_ref, keep_ref, row0, sem):
    copies = []
    for k in range(SLABS):
        source = scr.at[pl.ds(pl.multiple_of((me ^ k) * SROWS, 16), SROWS), :]
        target = (send_ref if k % 2 else keep_ref).at[k // 2, pl.ds(row0, SROWS), :]
        copies.append(pltpu.make_async_copy(source, target, sem.at[k]))
    return copies


def pairs_kernel(meta_ref, *refs, groups, total):
    count = len(groups)
    send_ref, keep_ref, scr, sem = refs[2 * count :]
    me = meta_ref[2]
    step = 0
    waiting = {}
    for g, blocks in enumerate(groups):
        left_ref, right_ref = refs[2 * g], refs[2 * g + 1]
        width = scr.shape[2]
        for b in range(blocks):
            slot = step % 2
            if step >= 2:
                for copy in waiting[step - 2]:
                    copy.wait()
            scr[slot] = dot(left_ref[...], right_ref[:, width * b : width * (b + 1)], TN).astype(BF)
            waiting[step] = slabs_out(
                scr.at[slot], me, send_ref, keep_ref, step * SROWS, sem.at[slot]
            )
            for copy in waiting[step]:
                copy.start()
            step += 1
    for late in (total - 2, total - 1):
        if late >= 0:
            for copy in waiting[late]:
                copy.wait()


def pair_grads(meta, pairs, width, column=None):
    groups = tuple(1 if column is not None else r.shape[1] // width for _, r in pairs)
    total = sum(groups)
    flat = [a for pair in pairs for a in pair]
    left_spec = full((LEN, D))
    specs = []
    for _, right in pairs:
        specs.append(left_spec)
        if column is None:
            specs.append(full(right.shape))
        else:
            specs.append(
                pl.BlockSpec((LEN, width), lambda i: (0, column), pipeline_mode=pl.Buffered(1))
            )
    return pl.pallas_call(
        functools.partial(pairs_kernel, groups=groups, total=total),
        grid=(1,),
        in_specs=[SMEM] + specs,
        out_specs=[ANY, ANY],
        out_shape=[sds(4, total * SROWS, width)] * 2,
        scratch_shapes=[pltpu.VMEM((2, D, width), BF), pltpu.SemaphoreType.DMA((2, SLABS))],
        cost_estimate=cost(2 * LEN * D * width * total * 1.2, 15e6),
        name="pair_grads",
    )(meta, *flat)


def down_kernel(meta_ref, act_ref, db_ref, out_ref):
    out_ref[0] = dot(act_ref[...], db_ref[...], TN).astype(BF)


def down_grads(meta, act, db, parity):
    wide = FF // SLABS
    return pl.pallas_call(
        down_kernel,
        grid_spec=pltpu.PrefetchScalarGridSpec(
            num_scalar_prefetch=1,
            grid=(4,),
            in_specs=[
                pl.BlockSpec((LEN, wide), lambda i, m: (0, m[2] ^ (2 * i + parity))),
                pl.BlockSpec((LEN, D), lambda i, m: (0, 0), pipeline_mode=pl.Buffered(1)),
            ],
            out_specs=pl.BlockSpec((1, wide, D), lambda i, m: (i, 0, 0)),
        ),
        out_shape=sds(4, wide, D),
        cost_estimate=cost(LEN * FF * D * 1.2, 7e6),
        name="down_grads",
    )(meta, act, db)


def swap(value, axis, bit, size):
    return lax.ppermute(value, axis, [(i, i ^ bit) for i in range(size)])


def gather_begin(halves):
    return [{0: halves[0]}, {0: halves[1]}]


def gather_stage(held, stage):
    for h, (near, far) in enumerate(((2, 4), (4, 2))):
        mine = held[h]
        if stage < 2:
            bit = (near, far)[stage]
            mine.update({k ^ bit: swap(mine[k], "shard", bit, 8) for k in list(mine) if k % 2 == 0})
        fresh = [k for k in mine if k % 2 == 0 and k ^ 1 not in mine]
        fresh = [k for k in fresh if stage == 2 or not k & (near, far)[stage]]
        mine.update({k ^ 1: swap(mine[k], "shard", 1, 8) for k in fresh})
    return held


def gathered(held):
    return [held[h][k] for k in range(8) for h in range(2)]


def add(*terms):
    return sum(t.astype(F32) for t in terms).astype(BF)


class Reduction:
    def __init__(self, send, keep, place):
        self.keep, self.place, self.stage = keep, place, 0
        self.got = swap(send, "shard", 1, 8)
        self.half = send.shape[1] // 2
        self.cuts = (
            (slice(0, self.half), 2, 4, (1, 3), (0, 2)),
            (slice(self.half, None), 4, 2, (2, 3), (0, 1)),
        )

    def step(self):
        self.stage += 1
        return (self.near, self.far, self.across, self.share)[self.stage - 1]()

    def near(self):
        sent = []
        self.back = []
        for cut, first, _, out, _ in self.cuts:
            away = jnp.stack([add(self.keep[p, cut], self.got[p, cut]) for p in out])
            sent.append(away)
            self.back.append(swap(away, "shard", first, 8))
        return sent

    def far(self):
        sent = []
        self.last = []
        for (cut, _, second, _, stay), back in zip(self.cuts, self.back):
            away = add(self.keep[stay[1], cut], self.got[stay[1], cut], back[1])
            sent.append(away)
            self.last.append(swap(away, "shard", second, 8))
        return sent

    def across(self):
        ends = [
            add(self.keep[0, cut[0]], self.got[0, cut[0]], back[0], last)
            for cut, back, last in zip(self.cuts, self.back, self.last)
        ]
        value = jnp.concatenate(ends)
        self.shape = value.shape
        parts = value.reshape(4, value.shape[0] // 4, value.shape[1])
        own, *sent = [
            lax.dynamic_index_in_dim(parts, self.place ^ k, 0, False) for k in range(4)
        ]
        self.terms = [own] + [swap(p, "rep", k, 4) for k, p in zip((1, 2, 3), sent)]
        return [own] + sent

    def share(self):
        self.total = add(*self.terms)
        self.others = [swap(self.total, "rep", k, 4) for k in (1, 2, 3)]
        return [self.total]

    def result(self):
        quarter = self.shape[0] // 4
        out = jnp.zeros((4, quarter, self.shape[1]), F32)
        for k, part in enumerate([self.total] + self.others):
            out = lax.dynamic_update_index_in_dim(out, part.astype(F32), self.place ^ k, 0)
        return out.reshape(self.shape)


def after(meta, *values):
    return lax.optimization_barrier((meta,) + values)[0]


def whole_slabs(send, keep):
    return jnp.stack([keep, send], axis=1).reshape((SLABS,) + send.shape[1:])


def reduce_any(matrix):
    share = lax.psum_scatter(matrix, "shard", scatter_dimension=0, tiled=True)
    return lax.psum(share, "rep").astype(F32)


def body(n_shard, n_rep, tokens, cotangent, lengths, dealing, drop_flags, *masters):
    matrices = [m.astype(BF) for m in masters[:6]]
    vectors = [m.astype(BF) for m in masters[6:]]
    permuted = n_shard == 8 and n_rep == 4
    position = lax.axis_index("shard")
    me = position if permuted else jnp.zeros((), jnp.int32)
    place = lax.axis_index("rep")
    length = lax.dynamic_index_in_dim(lengths[0], position, 0, False)
    flag = jnp.sum(jnp.where(dealing[0] == position, drop_flags[0], 0))
    meta = jnp.stack([length, flag, me]).astype(jnp.int32)
    x = tokens.reshape(LEN, D)
    cot = cotangent.reshape(LEN, D)

    names = vectors[:5] + vectors[6:9]
    width = D // n_shard
    small = jnp.concatenate([v[None] for v in names] + [vectors[5].reshape(4, width)])
    wq, wk, wv, wo, wu, wd = matrices
    if permuted:
        held = small[None]
        for bit in (1, 2, 4):
            held = jnp.concatenate([held, swap(held, "shard", bit, 8)])
        every = jnp.take(held, jnp.arange(8, dtype=jnp.int32) ^ position, axis=0)
        ups = [wu[:, D * j : D * (j + 1)] for j in range(4)]
        cuts = (slice(0, 48), slice(48, 96))
        near = gather_begin([jnp.concatenate([m[c] for m in (wq, wk, wv)]) for c in cuts])
        gather_stage(near, 0)
        gather_stage(near, 1)
        far_halves = [
            jnp.concatenate([m[c] for m in [wo] + ups] + [wd[c2]])
            for c, c2 in zip(cuts, (slice(0, 192), slice(192, 384)))
        ]
        far = gather_begin(
            lax.optimization_barrier(tuple(far_halves) + (near[0][6], near[1][6], held))[:2]
        )
        gather_stage(near, 2)
        near = gathered(near)
        gather_stage(far, 0)
    else:
        every = lax.all_gather(small, "shard", axis=0)
        whole = [lax.all_gather(m, "shard", axis=0, tiled=True) for m in matrices]
        near = [jnp.concatenate(whole[:3])]
        far = [
            jnp.concatenate(
                [whole[3]] + [whole[4][:, D * j : D * (j + 1)] for j in range(4)] + [whole[5]]
            )
        ]
    every = every.astype(F32)
    vec = every[:, :8].transpose(1, 0, 2).reshape(8, D)
    ub = every[:, 8:].reshape(1, FF)
    ub = jnp.broadcast_to(ub, (8, FF))

    q, k, v = qkv(meta, x, vec, near)
    heads = attend(meta, q, k, v, (), 0, 2)
    if permuted:
        gather_stage(far, 1)
        m = after(meta, heads[0], far[0][2], far[1][4])
    else:
        m = after(meta, heads[0])
    heads = attend(m, q, k, v, heads, 2, 4)
    ctx, aug = heads
    if permuted:
        gather_stage(far, 2)
        far = gathered(far)
    output, first, act, slope, n1, inv, db, sums = mid1(meta, x, ctx, cot, vec, ub, far)
    jobs = []

    def begin(send, keep):
        if permuted:
            jobs.append(Reduction(send, keep, place))

    def step(index):
        return tuple(jobs[index].step()) if permuted else ()

    d_send = down_grads(meta, act, db, 1)
    d_keep = down_grads(after(meta, d_send), act, db, 0)
    begin(d_send, d_keep)
    m = after(meta, d_keep, *step(0))
    dh, da, dctx, sums = mid2(m, db, slope, n1, inv, vec, sums, far)
    m = after(meta, dctx, *step(0))
    u_send, u_keep = pair_grads(m, ((first, dh), (ctx, da)), D)
    begin(u_send, u_keep)
    m = after(meta, u_keep, *step(0))
    *grads, sums = attend_back(m, aug, k, v, ctx, dctx, sums, (), 0, 2)
    m = after(meta, sums, *step(1), *step(0))
    *grads, sums = attend_back(m, aug, k, v, ctx, dctx, sums, grads, 2, 2)
    m = after(meta, sums, *step(1))
    a_send, a_keep = pair_grads(m, [(x, g) for g in grads], 512, 0)
    begin(a_send, a_keep)
    m = after(meta, a_keep)
    *grads, sums = attend_back(m, aug, k, v, ctx, dctx, sums, grads, 4, 2)
    m = after(meta, sums, *step(1), *step(2))
    b_send, b_keep = pair_grads(m, [(x, g) for g in grads], 256, 2)
    begin(b_send, b_keep)
    m = after(meta, b_keep, *step(2))
    grad_x = input_grad(m, da, *grads, cot, near)

    if permuted:
        for bit in (1, 2, 4):
            sums = sums + swap(sums, "shard", bit, 8)
        for bit in (1, 2):
            sums = sums + swap(sums, "rep", bit, 4)
    else:
        sums = lax.psum(sums, ("rep", "shard"))
    grads_v = lax.dynamic_index_in_dim(sums[:8].reshape(8, n_shard, width), position, 1, False)
    grad_ub = lax.dynamic_index_in_dim(sums[8:12].reshape(n_shard, FF // n_shard), position, 0, False)

    if permuted:
        step(3)
        step(3)
        step(2)
        step(3)
        step(1)
        step(2)
        step(3)
        grad_down, g_uo, g_a, g_b = (job.result() for job in jobs)
        grad_up = jnp.concatenate([g_uo[96 * j : 96 * (j + 1)] for j in range(4)], axis=1)
        grad_out = g_uo[384:]
        grad_qkv = [
            jnp.concatenate([g[96 * j : 96 * (j + 1)] for g in (g_a, g_b)], axis=1)
            for j in range(3)
        ]
    else:
        def rebuild(slabs, j):
            return slabs[:, SROWS * j : SROWS * (j + 1)].reshape(D, slabs.shape[2])

        grad_down = reduce_any(whole_slabs(d_send, d_keep).reshape(FF, D))
        g_uo = whole_slabs(u_send, u_keep)
        g_a = whole_slabs(a_send, a_keep)
        g_b = whole_slabs(b_send, b_keep)
        grad_up = reduce_any(jnp.concatenate([rebuild(g_uo, j) for j in range(4)], axis=1))
        grad_out = reduce_any(rebuild(g_uo, 4))
        grad_qkv = [
            reduce_any(jnp.concatenate([rebuild(g, j) for g in (g_a, g_b)], axis=1))
            for j in range(3)
        ]
    return (
        output.reshape(tokens.shape),
        grad_x.reshape(tokens.shape),
        grad_qkv[0],
        grad_qkv[1],
        grad_qkv[2],
        grad_out,
        grad_up,
        grad_down,
        grads_v[0],
        grads_v[1],
        grads_v[2],
        grads_v[3],
        grads_v[4],
        grad_ub,
        grads_v[5],
        grads_v[6],
        grads_v[7],
    )


def solution(mesh):
    tokens = P(("rep", "shard"), None, None)
    table = P("rep", None)
    matrix = P("shard", None)
    vector = P("shard")
    return jax.shard_map(
        functools.partial(body, mesh.shape["shard"], mesh.shape["rep"]),
        mesh=mesh,
        in_specs=(tokens, tokens) + (table,) * 3 + (matrix,) * 6 + (vector,) * 9,
        out_specs=(tokens, tokens) + (matrix,) * 6 + (vector,) * 9,
        check_vma=False,
    )
```
